8 devices in a mesh: dp: 1 (over z), t: 2 (over y), stage: 4 (over x, core).
Axes of the slice: x: 2, y: 2, z: 1, core: 2. Of those that a mesh axis runs over, the one named last changes fastest.
Arguments:
- hidden: bfloat16 [4, 24, 1536, 2048], P(('dp', 'stage'))
- w_query: bfloat16 [2048, 3072], P(None, 't')
- w_dkv: bfloat16 [2048, 576], replicated
- latent_gain: bfloat16 [512], replicated
- w_uk: bfloat16 [512, 2048], P(None, 't')
- w_uv: bfloat16 [512, 2048], P(None, 't')
- w_out: bfloat16 [2048, 2048], P('t')
Outputs:
- output 1: bfloat16 [4, 24, 1536, 2048], P(('dp', 'stage'))
- output 2: bfloat16 [4, 24, 1536, 576], P(('dp', 'stage'), 't')
All inputs are finite; a program needn't handle non-finite values.
Results may differ from the reference program's by a relative error of at most 0.00897654.
Values are sent between devices in bfloat16 or wider.
A program may use at most 1.5 GiB of HBM per device.

```python
import jax
import jax.numpy as jnp
from jax import lax

D_MODEL = 2048
HEADS = 16
KV_RANK = 512
ROPE_DIM = 64
NOPE_DIM = 128
V_DIM = 128
STAGE_SLOTS = 4
REQUESTS = 24
SEQ_LEN = 1536

NORM_EPS = 1e-6
ROPE_BASE = 10000.0
HALF_ROPE = ROPE_DIM // 2
HEAD_DIM = NOPE_DIM + ROPE_DIM
PROMPT_SLOTS = STAGE_SLOTS // 2
N_BLOCKS = max(1, min(8, SEQ_LEN // 128))
BLOCK_LEN = SEQ_LEN // N_BLOCKS


def setup_inputs(seed: int = 0, part: int = 0) -> dict:
    part_key = jax.random.fold_in(jax.random.key(seed), part)
    shared = jax.random.split(jax.random.key(seed + 1), 6)
    hidden = jax.random.normal(part_key, (STAGE_SLOTS, REQUESTS, SEQ_LEN, D_MODEL), jnp.float32).astype(jnp.bfloat16)
    w_query = (jax.random.normal(shared[0], (D_MODEL, HEADS * HEAD_DIM), jnp.float32) * D_MODEL ** -0.5).astype(jnp.bfloat16)
    w_dkv = (jax.random.normal(shared[1], (D_MODEL, KV_RANK + ROPE_DIM), jnp.float32) * D_MODEL ** -0.5).astype(jnp.bfloat16)
    latent_gain = (1.0 + 0.3 * jax.random.normal(shared[2], (KV_RANK,), jnp.float32)).astype(jnp.bfloat16)
    w_uk = (jax.random.normal(shared[3], (KV_RANK, HEADS * NOPE_DIM), jnp.float32) * KV_RANK ** -0.5).astype(jnp.bfloat16)
    w_uv = (jax.random.normal(shared[4], (KV_RANK, HEADS * V_DIM), jnp.float32) * KV_RANK ** -0.5).astype(jnp.bfloat16)
    w_out = (jax.random.normal(shared[5], (HEADS * V_DIM, D_MODEL), jnp.float32) * (HEADS * V_DIM) ** -0.5).astype(jnp.bfloat16)
    return {"hidden": hidden, "w_query": w_query, "w_dkv": w_dkv, "latent_gain": latent_gain, "w_uk": w_uk, "w_uv": w_uv, "w_out": w_out}


def rope_tables():
    positions = jnp.arange(SEQ_LEN).astype(jnp.float32)
    inv_freq = ROPE_BASE ** (-jnp.arange(HALF_ROPE).astype(jnp.float32) / HALF_ROPE)
    angles = positions[:, None] * inv_freq[None, :]
    return jnp.cos(angles), jnp.sin(angles)


def apply_rope(vecs, cos_tab, sin_tab):
    as_f32 = vecs.astype(jnp.float32)
    low_half = as_f32[..., :HALF_ROPE]
    high_half = as_f32[..., HALF_ROPE:]
    rotated = jnp.concatenate([low_half * cos_tab - high_half * sin_tab, high_half * cos_tab + low_half * sin_tab], axis=-1)
    return rotated.astype(jnp.bfloat16)


def reference(hidden, w_query, w_dkv, latent_gain, w_uk, w_uv, w_out):
    cos_tab, sin_tab = rope_tables()

    def one_request(tokens):
        compressed = jnp.dot(tokens, w_dkv, preferred_element_type=jnp.float32).astype(jnp.bfloat16)
        c_raw = compressed[:, :KV_RANK].astype(jnp.float32)
        inv_rms = lax.rsqrt(jnp.mean(c_raw * c_raw, axis=-1, keepdims=True) + NORM_EPS)
        c_kv = (c_raw * inv_rms * latent_gain.astype(jnp.float32)).astype(jnp.bfloat16)
        k_rope = apply_rope(compressed[:, KV_RANK:], cos_tab, sin_tab)
        queries = jnp.dot(tokens, w_query, preferred_element_type=jnp.float32).astype(jnp.bfloat16)
        queries = queries.reshape(SEQ_LEN, HEADS, HEAD_DIM)
        q_nope = queries[:, :, :NOPE_DIM].astype(jnp.float32)
        q_rope = apply_rope(queries[:, :, NOPE_DIM:], cos_tab[:, None, :], sin_tab[:, None, :]).astype(jnp.float32)
        k_nope = jnp.dot(c_kv, w_uk, preferred_element_type=jnp.float32).astype(jnp.bfloat16)
        k_nope = k_nope.reshape(SEQ_LEN, HEADS, NOPE_DIM).astype(jnp.float32)
        values = jnp.dot(c_kv, w_uv, preferred_element_type=jnp.float32).astype(jnp.bfloat16)
        values = values.reshape(SEQ_LEN, HEADS, V_DIM).astype(jnp.float32)
        k_rope_f = k_rope.astype(jnp.float32)
        pieces = []
        for block_idx in range(N_BLOCKS):
            start_row = block_idx * BLOCK_LEN
            stop_row = start_row + BLOCK_LEN
            scores = jnp.einsum("qhe,khe->hqk", q_nope[start_row:stop_row], k_nope[:stop_row])
            scores = scores + jnp.einsum("qhe,ke->hqk", q_rope[start_row:stop_row], k_rope_f[:stop_row])
            q_pos = start_row + jnp.arange(BLOCK_LEN)[:, None]
            k_pos = jnp.arange(stop_row)[None, :]
            scores = jnp.where(k_pos <= q_pos, scores * HEAD_DIM ** -0.5, -jnp.inf)
            row_peak = jnp.max(scores, axis=-1, keepdims=True)
            weights = jnp.exp(scores - row_peak)
            row_total = jnp.sum(weights, axis=-1)
            mixed = jnp.einsum("hqk,khe->qhe", weights.astype(jnp.bfloat16).astype(jnp.float32), values[:stop_row])
            pieces.append((mixed / row_total.T[:, :, None]).astype(jnp.bfloat16))
        head_mix = jnp.concatenate(pieces, axis=0).reshape(SEQ_LEN, HEADS * V_DIM)
        out_rows = jnp.dot(head_mix, w_out, preferred_element_type=jnp.float32).astype(jnp.bfloat16)
        latent = jnp.concatenate([c_kv, k_rope], axis=-1)
        return out_rows, latent

    prompts = hidden[:PROMPT_SLOTS].reshape(PROMPT_SLOTS * REQUESTS, SEQ_LEN, D_MODEL)
    out_rows, latent = lax.map(one_request, prompts)
    out_rows = out_rows.reshape(PROMPT_SLOTS, REQUESTS, SEQ_LEN, D_MODEL)
    latent = latent.reshape(PROMPT_SLOTS, REQUESTS, SEQ_LEN, KV_RANK + ROPE_DIM)
    attn_out = jnp.concatenate([out_rows, jnp.zeros_like(out_rows)], axis=0)
    latent_cache = jnp.concatenate([jnp.zeros_like(latent), latent], axis=0)
    return attn_out, latent_cache
```

```python
import functools
import math

import jax
import jax.numpy as jnp
from jax import lax
from jax.experimental import pallas as pl
from jax.experimental.layout import Layout, with_layout_constraint
from jax.experimental.pallas import tpu as pltpu
from jax.sharding import PartitionSpec as P


NOPE_DIM = 128
ROPE_DIM = 64
HALF_ROPE = ROPE_DIM // 2
NORM_EPS = 1e-6
ROPE_BASE = 10000.0
BLOCK = 256
LANES = 128


N_FAR = 7
N_SWAP = 1
STEP_CALLS = (1, 1, 1, 1, 1, 1, 1)
TAIL_CALLS = (1, 1)


def rope_tables(seq_len):
    positions = jnp.arange(seq_len, dtype=jnp.float32)
    inv_freq = ROPE_BASE ** (-jnp.arange(HALF_ROPE, dtype=jnp.float32) / HALF_ROPE)
    angles = positions[:, None] * inv_freq[None, :]
    cos_tab, sin_tab = jnp.cos(angles), jnp.sin(angles)
    reps = LANES // ROPE_DIM
    return jnp.tile(cos_tab, (1, 2 * reps)), jnp.tile(jnp.concatenate([-sin_tab, sin_tab], axis=1), (1, reps))


def attend_kernel(n_ret, aliased, ids, flags, hid, recv, w_dkv, gain, wq_own, wq_oth, kvo_own, kvo_oth, cos_ref, sin_ref, *rest):
    if aliased:
        rest = rest[1:]
    if n_ret:
        out_ref, lat_ref, ret_ref, *scratch = rest
    else:
        out_ref, lat_ref, *scratch = rest
        ret_ref = None
    x_s, k_s, v_s, kr_s, q_s, qr_s, o_s, s0_s, s1_s, p0_s, p1_s, t0_s, t1_s = scratch
    req, blk = pl.program_id(0), pl.program_id(1)
    n_blocks = k_s.shape[0] // BLOCK
    kv_rank = gain.shape[1]
    half = kvo_own.shape[1] // 2
    n_heads = k_s.shape[1] // NOPE_DIM
    is_far = flags[0] == 1
    active = flags[1 + req] == 1
    scale = (NOPE_DIM + ROPE_DIM) ** -0.5 * math.log2(math.e)

    def rope(vecs):
        lane = lax.broadcasted_iota(jnp.int32, (BLOCK, LANES), 1)
        low = lane % ROPE_DIM < HALF_ROPE
        cos_tab, sin_tab = cos_ref[...], sin_ref[...]
        parts = []
        for start in range(0, vecs.shape[1], LANES):
            vec = vecs[:, start:start + LANES].astype(jnp.float32)
            other = jnp.where(low, pltpu.roll(vec, LANES - HALF_ROPE, 1), pltpu.roll(vec, HALF_ROPE, 1))
            parts.append((vec * cos_tab + other * sin_tab).astype(jnp.bfloat16))
        return jnp.concatenate(parts, axis=1)

    @pl.when(active)
    def _():
        @pl.when(is_far)
        def _():
            x_s[...] = recv[0]

        @pl.when(jnp.logical_not(is_far))
        def _():
            x_s[...] = hid[0]

        rows = pl.ds(pl.multiple_of(blk * BLOCK, BLOCK), BLOCK)
        comp = jnp.dot(x_s[...], w_dkv[...], preferred_element_type=jnp.float32).astype(jnp.bfloat16)
        raw = comp[:, :kv_rank].astype(jnp.float32)
        inv_rms = lax.rsqrt(jnp.mean(raw * raw, axis=-1, keepdims=True) + NORM_EPS)
        c_kv = (raw * inv_rms * gain[...]).astype(jnp.bfloat16)
        k_rope = rope(comp[:, kv_rank:])
        kr_s[rows, :] = k_rope
        lat_ref[0, :, :kv_rank] = c_kv
        lat_ref[0, :, kv_rank:] = k_rope[:, :ROPE_DIM]
        for idx, (wq, kvo) in enumerate(((wq_own, kvo_own), (wq_oth, kvo_oth))):
            cols = slice(idx * half, (idx + 1) * half)
            k_s[rows, cols] = jnp.dot(c_kv, kvo[:kv_rank, :half], preferred_element_type=jnp.float32).astype(jnp.bfloat16)
            v_s[rows, cols] = jnp.dot(c_kv, kvo[:kv_rank, half:], preferred_element_type=jnp.float32).astype(jnp.bfloat16)
            q_s[:, cols] = jnp.dot(x_s[...], wq[:, :half], preferred_element_type=jnp.float32).astype(jnp.bfloat16)
            q_rope = jnp.dot(x_s[...], wq[:, half:], preferred_element_type=jnp.float32).astype(jnp.bfloat16)
            qr_s[:, idx * half // 2:(idx + 1) * half // 2] = rope(q_rope)

        for step in range(n_blocks):
            @pl.when(blk == step)
            def _(step=step):
                prev = step * BLOCK
                length = prev + BLOCK
                causal = lax.broadcasted_iota(jnp.int32, (BLOCK, BLOCK), 1) <= lax.broadcasted_iota(jnp.int32, (BLOCK, BLOCK), 0)

                def score(head, odd, dst):
                    cols = pl.ds(pl.multiple_of(head * NOPE_DIM, NOPE_DIM), NOPE_DIM)
                    thin = pl.ds(pl.multiple_of(head // 2 * LANES, LANES), LANES)
                    query = jnp.concatenate([q_s[:, cols], qr_s[:, thin]], axis=1)
                    keys = jnp.concatenate([k_s[:length, cols], kr_s[:length, odd * LANES:(odd + 1) * LANES]], axis=1)
                    dst[:, :length] = lax.dot_general(query, keys, (((1,), (1,)), ((), ())), preferred_element_type=jnp.float32)

                def weigh(src, dst, total_ref):
                    diag = jnp.where(causal, src[:, prev:length], -jnp.inf)
                    peak = jnp.max(diag, axis=-1, keepdims=True)
                    if prev:
                        peak = jnp.maximum(peak, jnp.max(src[:, :prev], axis=-1, keepdims=True))
                    e_diag = jnp.exp2((diag - peak) * scale)
                    total = jnp.sum(e_diag, axis=-1, keepdims=True)
                    dst[:, prev:length] = e_diag.astype(jnp.bfloat16)
                    if prev:
                        e_past = jnp.exp2((src[:, :prev] - peak) * scale)
                        total = total + jnp.sum(e_past, axis=-1, keepdims=True)
                        dst[:, :prev] = e_past.astype(jnp.bfloat16)
                    total_ref[...] = jnp.broadcast_to(total, total_ref.shape)

                def mix(head, src, total_ref):
                    cols = pl.ds(pl.multiple_of(head * NOPE_DIM, NOPE_DIM), NOPE_DIM)
                    mixed = jnp.dot(src[:, :length], v_s[:length, cols], preferred_element_type=jnp.float32)
                    o_s[:, cols] = (mixed / total_ref[...]).astype(jnp.bfloat16)

                def pair(idx, carry):
                    head = idx * 2
                    score(head + 1, 1, s1_s)
                    weigh(s0_s, p0_s, t0_s)
                    mix(jnp.maximum(head - 1, 0), p1_s, t1_s)
                    score(jnp.minimum(head + 2, n_heads - 2), 0, s0_s)
                    weigh(s1_s, p1_s, t1_s)
                    mix(head, p0_s, t0_s)
                    return carry

                score(0, 0, s0_s)
                lax.fori_loop(0, n_heads // 2, pair, 0)
                mix(n_heads - 1, p1_s, t1_s)

        y = jnp.dot(o_s[:, :half], kvo_own[kv_rank:, :], preferred_element_type=jnp.float32)
        y = y + jnp.dot(o_s[:, half:], kvo_oth[kv_rank:, :], preferred_element_type=jnp.float32)
        y = y.astype(jnp.bfloat16)
        if ret_ref is not None:
            @pl.when(req < n_ret)
            def _():
                ret_ref[0] = y

        @pl.when(jnp.logical_not(is_far))
        def _():
            out_ref[0] = y

    @pl.when(jnp.logical_not(jnp.logical_and(active, jnp.logical_not(is_far))))
    def _():
        out_ref[0] = jnp.zeros(out_ref.shape[1:], out_ref.dtype)


def attend(ids, flags, hidden, recv, weights, out_prev, n_ret):
    n_req = ids.shape[0]
    _, seq_len, width = hidden.shape
    w_dkv, gain, wq_own, wq_oth, kvo_own, kvo_oth, _, _ = weights
    n_blocks = seq_len // BLOCK
    kv_rank = gain.shape[1]
    half = kvo_own.shape[1] // 2
    lat_width = kv_rank + ROPE_DIM
    whole = lambda arr: pl.BlockSpec(arr.shape, lambda r, i, ids, flags: (0, 0), pipeline_mode=pl.Buffered(1))
    in_specs = [
        pl.BlockSpec((1, BLOCK, width), lambda r, i, ids, flags: (jnp.where(flags[0] == 1, 0, ids[r]), jnp.where(flags[0] == 1, 0, i), 0)),
        pl.BlockSpec((1, BLOCK, width), lambda r, i, ids, flags: (0, jnp.where((flags[0] == 1) & (r == 0), i, 0), 0)),
        *[whole(arr) for arr in (w_dkv, gain, wq_own, wq_oth, kvo_own, kvo_oth)],
        pl.BlockSpec((BLOCK, LANES), lambda r, i, ids, flags: (i, 0)),
        pl.BlockSpec((BLOCK, LANES), lambda r, i, ids, flags: (i, 0)),
    ]
    args = [hidden, recv, *weights]
    out_shape = [jax.ShapeDtypeStruct(hidden.shape, jnp.bfloat16), jax.ShapeDtypeStruct((n_req, seq_len, lat_width), jnp.bfloat16)]
    out_specs = [
        pl.BlockSpec((1, BLOCK, width), lambda r, i, ids, flags: (ids[r], i, 0)),
        pl.BlockSpec((1, BLOCK, lat_width), lambda r, i, ids, flags: (r, i, 0)),
    ]
    if n_ret:
        out_shape.append(jax.ShapeDtypeStruct((n_ret, seq_len, width), jnp.bfloat16))
        out_specs.append(pl.BlockSpec((1, BLOCK, width), lambda r, i, ids, flags: (jnp.minimum(r, n_ret - 1), jnp.where(r < n_ret, i, n_blocks - 1), 0)))
    aliases = {}
    if out_prev is not None:
        in_specs.append(pl.BlockSpec(memory_space=pl.ANY))
        args.append(out_prev)
        aliases = {2 + len(args) - 1: 0}
    flops = n_req * seq_len * (2 * width * (768 + 3 * half * 2 // 2 * 1 + 2 * half) + 8 * kv_rank * half + 2 * half * seq_len * 3)
    outs = pl.pallas_call(
        functools.partial(attend_kernel, n_ret, out_prev is not None),
        out_shape=out_shape,
        grid_spec=pltpu.PrefetchScalarGridSpec(
            num_scalar_prefetch=2,
            grid=(n_req, n_blocks),
            in_specs=in_specs,
            out_specs=out_specs,
            scratch_shapes=[
                pltpu.VMEM((BLOCK, width), jnp.bfloat16),
                pltpu.VMEM((seq_len, 2 * half), jnp.bfloat16),
                pltpu.VMEM((seq_len, 2 * half), jnp.bfloat16),
                pltpu.VMEM((seq_len, 2 * LANES), jnp.bfloat16),
                pltpu.VMEM((BLOCK, 2 * half), jnp.bfloat16),
                pltpu.VMEM((BLOCK, half), jnp.bfloat16),
                pltpu.VMEM((BLOCK, 2 * half), jnp.bfloat16),
                *[pltpu.VMEM((BLOCK, seq_len), jnp.float32)] * 2,
                *[pltpu.VMEM((BLOCK, seq_len), jnp.bfloat16)] * 2,
                *[pltpu.VMEM((BLOCK, NOPE_DIM), jnp.float32)] * 2,
            ],
        ),
        input_output_aliases=aliases,
        compiler_params=pltpu.CompilerParams(dimension_semantics=("arbitrary", "arbitrary"), vmem_limit_bytes=66_000_000),
        cost_estimate=pl.CostEstimate(flops=flops, bytes_accessed=n_req * seq_len * width * 6, transcendentals=n_req * seq_len * seq_len * 8),
        name="attend",
    )(ids, flags, *args)
    return outs if n_ret else (*outs, None)


def solution(mesh):
    n_stage = mesh.shape["stage"]
    half_stage = n_stage // 2
    down = [(idx, idx + half_stage) for idx in range(half_stage)]
    up = [(idx + half_stage, idx) for idx in range(half_stage)]
    cores = [(idx, idx ^ 1) for idx in range(n_stage)]
    swap = [(0, 1), (1, 0)]
    slot_spec = P(("dp", "stage"), None, None, None)
    cache_spec = P(("dp", "stage"), "t", None, None)

    def other_half(arr, core):
        rows = arr.shape[0] // 2
        mine = lax.ppermute(lax.dynamic_slice_in_dim(arr, core * rows, rows, axis=0), "t", swap)
        theirs = lax.ppermute(mine, "stage", cores)
        first = jnp.where(core == 0, mine, theirs)
        second = jnp.where(core == 0, theirs, mine)
        return jnp.concatenate([first, second], axis=0)

    def device_step(hidden, w_query, w_dkv, latent_gain, w_uk, w_uv, w_out):
        tokens = hidden[0]
        n_all, seq_len, width = tokens.shape
        kv_rank = latent_gain.shape[0]
        n_half = n_all // 2
        t_index = lax.axis_index("t")
        stage = lax.axis_index("stage")
        is_prompt = stage < half_stage
        core = stage % 2
        own, oth = t_index * n_half, (1 - t_index) * n_half

        arrivals = []
        for idx in range(N_FAR):
            index = own + idx
            if arrivals:
                index, _ = lax.optimization_barrier((index, arrivals[-1]))
            piece = lax.dynamic_slice_in_dim(tokens, index, 1, axis=0)
            arrivals.append(lax.ppermute(piece, "stage", down))

        heads_here = w_uk.shape[1] // NOPE_DIM
        wq = w_query.reshape(width, heads_here, NOPE_DIM + ROPE_DIM)
        wq_own = jnp.concatenate([wq[:, :, :NOPE_DIM].reshape(width, -1), wq[:, :, NOPE_DIM:].reshape(width, -1)], axis=1)
        kvo_own = jnp.concatenate([jnp.concatenate([w_uk, w_uv], axis=1), w_out], axis=0)
        wq_oth, kvo_oth = other_half(wq_own, core), other_half(kvo_own, core)
        blank = jnp.zeros((width, ROPE_DIM), w_dkv.dtype)
        w_dkv_wide = jnp.concatenate([w_dkv, blank, blank, w_dkv[:, kv_rank:]], axis=1)
        gain = latent_gain.astype(jnp.float32)[None, :]
        weights = (w_dkv_wide, gain, wq_own, wq_oth, kvo_own, kvo_oth, *rope_tables(seq_len))

        ids = jnp.concatenate([own + jnp.arange(N_FAR, n_half), oth + jnp.arange(N_FAR + N_SWAP, n_half)]).astype(jnp.int32)
        far = jnp.where(is_prompt, 0, 1).astype(jnp.int32)
        place = lambda out, block, index: lax.dynamic_update_slice(out, jnp.where(is_prompt, block, jnp.zeros_like(block)), (index, 0, 0))

        out, done = None, 0
        latents, far_latents = [], []
        backs, movements = {}, {}

        def put(idx, source):
            nonlocal out
            for block, index in source.pop(idx, ()):
                out = place(out, block, index)

        def run(count, recv, n_ret, far_active):
            nonlocal out, done
            flags = jnp.stack([far, *[jnp.where(is_prompt, 1, 1 if far_active and idx == 0 else 0).astype(jnp.int32) for idx in range(count)]])
            out, lat, ret = attend(ids[done:done + count], flags, tokens, recv, weights, out, n_ret)
            n_send = max(0, min(count, n_half - N_FAR - done))
            if n_send:
                sent, _ = lax.optimization_barrier((lat[:n_send], arrivals[-1]))
                latents.append(lax.ppermute(sent, "stage", down))
            if far_active:
                far_latents.append(lat[:1])
            done += count
            return ret

        n_steps = len(STEP_CALLS)
        for idx, count in enumerate(STEP_CALLS):
            put(idx - 2, backs)
            put(idx - 4, movements)
            ret = run(count, arrivals[idx], 1, True)
            if idx < N_SWAP:
                swapped = lax.ppermute(ret, "t", swap)
            back = lax.ppermute(ret, "stage", up)
            moved = lax.ppermute(back, "t", swap)
            backs[idx] = [(back, own + idx)]
            movements[idx] = [(moved, oth + idx)]
            if idx < N_SWAP:
                movements[idx].append((swapped, oth + N_FAR + idx))
        for idx, count in enumerate(TAIL_CALLS):
            put(n_steps + idx - 2, backs)
            put(n_steps + idx - 4, movements)
            run(count, tokens, 0, False)
        for idx in range(n_steps):
            put(idx, backs)
            put(idx, movements)
        pieces = [*far_latents, *latents]

        def empty(parts):
            return with_layout_constraint(jnp.zeros((n_half, kv_rank + ROPE_DIM, seq_len), jnp.bfloat16), Layout((0, 1, 2)))

        def gathered(parts):
            return with_layout_constraint(jnp.swapaxes(jnp.concatenate(parts, axis=0), 1, 2), Layout((0, 1, 2)))

        latent = jnp.swapaxes(lax.cond(is_prompt, empty, gathered, pieces), 1, 2)
        return out[None], latent[None]

    in_specs = (slot_spec, P(None, "t"), P(None, None), P(None), P(None, "t"), P(None, "t"), P("t", None))
    return jax.shard_map(device_step, mesh=mesh, in_specs=in_specs, out_specs=(slot_spec, cache_spec), check_vma=False)
```

```python
import functools
import math

import jax
import jax.numpy as jnp
from jax import lax
from jax.experimental import pallas as pl
from jax.experimental.layout import Layout, with_layout_constraint
from jax.experimental.pallas import tpu as pltpu
from jax.sharding import PartitionSpec as P


NOPE_DIM = 128
ROPE_DIM = 64
HALF_ROPE = ROPE_DIM // 2
NORM_EPS = 1e-6
ROPE_BASE = 10000.0
BLOCK = 256
LANES = 128


N_FAR = 7
N_SWAP = 1
STEP_CALLS = (1, 1, 1, 1, 1, 1, 1)
TAIL_CALLS = (1, 1)


def rope_tables(seq_len):
    positions = jnp.arange(seq_len, dtype=jnp.float32)
    inv_freq = ROPE_BASE ** (-jnp.arange(HALF_ROPE, dtype=jnp.float32) / HALF_ROPE)
    angles = positions[:, None] * inv_freq[None, :]
    cos_tab, sin_tab = jnp.cos(angles), jnp.sin(angles)
    reps = LANES // ROPE_DIM
    return jnp.tile(cos_tab, (1, 2 * reps)), jnp.tile(jnp.concatenate([-sin_tab, sin_tab], axis=1), (1, reps))


def attend_kernel(n_ret, aliased, ids, flags, hid, recv, w_dkv, gain, wq_own, wq_oth, kv_own, kv_oth, wo_own, wo_oth, cos_ref, sin_ref, *rest):
    if aliased:
        rest = rest[1:]
    if n_ret:
        out_ref, lat_ref, ret_ref, *scratch = rest
    else:
        out_ref, lat_ref, *scratch = rest
        ret_ref = None
    x_s, k_s, v_s, kr_s, q_s, qr_s, o_s, s0_s, s1_s, p0_s, p1_s, t0_s, t1_s = scratch
    req, blk = pl.program_id(0), pl.program_id(1)
    n_blocks = k_s.shape[0] // BLOCK
    kv_rank = gain.shape[1]
    half = wo_own.shape[0]
    n_heads = k_s.shape[1] // NOPE_DIM
    is_far = flags[0] == 1
    active = flags[1 + req] == 1
    scale = (NOPE_DIM + ROPE_DIM) ** -0.5 * math.log2(math.e)

    def rope(vecs):
        lane = lax.broadcasted_iota(jnp.int32, (BLOCK, LANES), 1)
        low = lane % ROPE_DIM < HALF_ROPE
        cos_tab, sin_tab = cos_ref[...], sin_ref[...]
        parts = []
        for start in range(0, vecs.shape[1], LANES):
            vec = vecs[:, start:start + LANES].astype(jnp.float32)
            other = jnp.where(low, pltpu.roll(vec, LANES - HALF_ROPE, 1), pltpu.roll(vec, HALF_ROPE, 1))
            parts.append((vec * cos_tab + other * sin_tab).astype(jnp.bfloat16))
        return jnp.concatenate(parts, axis=1)

    @pl.when(active)
    def _():
        @pl.when(is_far)
        def _():
            x_s[...] = recv[0]

        @pl.when(jnp.logical_not(is_far))
        def _():
            x_s[...] = hid[0]

        rows = pl.ds(pl.multiple_of(blk * BLOCK, BLOCK), BLOCK)
        comp = jnp.dot(x_s[...], w_dkv[...], preferred_element_type=jnp.float32).astype(jnp.bfloat16)
        raw = comp[:, :kv_rank].astype(jnp.float32)
        inv_rms = lax.rsqrt(jnp.mean(raw * raw, axis=-1, keepdims=True) + NORM_EPS)
        c_kv = (raw * inv_rms * gain[...]).astype(jnp.bfloat16)
        k_rope = rope(comp[:, kv_rank:])
        kr_s[rows, :] = k_rope
        lat_ref[0, :, :kv_rank] = c_kv
        lat_ref[0, :, kv_rank:] = k_rope[:, :ROPE_DIM]
        for idx, (wq, kv) in enumerate(((wq_own, kv_own), (wq_oth, kv_oth))):
            cols = slice(idx * half, (idx + 1) * half)
            k_s[rows, cols] = jnp.dot(c_kv, kv[:, :half], preferred_element_type=jnp.float32).astype(jnp.bfloat16)
            v_s[rows, cols] = jnp.dot(c_kv, kv[:, half:], preferred_element_type=jnp.float32).astype(jnp.bfloat16)
            q_s[:, cols] = jnp.dot(x_s[...], wq[:, :half], preferred_element_type=jnp.float32).astype(jnp.bfloat16)
            q_rope = jnp.dot(x_s[...], wq[:, half:], preferred_element_type=jnp.float32).astype(jnp.bfloat16)
            qr_s[:, idx * half // 2:(idx + 1) * half // 2] = rope(q_rope)

        for step in range(n_blocks):
            @pl.when(blk == step)
            def _(step=step):
                prev = step * BLOCK
                length = prev + BLOCK
                causal = lax.broadcasted_iota(jnp.int32, (BLOCK, BLOCK), 1) <= lax.broadcasted_iota(jnp.int32, (BLOCK, BLOCK), 0)

                def score(head, odd, dst):
                    cols = pl.ds(pl.multiple_of(head * NOPE_DIM, NOPE_DIM), NOPE_DIM)
                    thin = pl.ds(pl.multiple_of(head // 2 * LANES, LANES), LANES)
                    query = jnp.concatenate([q_s[:, cols], qr_s[:, thin]], axis=1)
                    keys = jnp.concatenate([k_s[:length, cols], kr_s[:length, odd * LANES:(odd + 1) * LANES]], axis=1)
                    dst[:, :length] = lax.dot_general(query, keys, (((1,), (1,)), ((), ())), preferred_element_type=jnp.float32)

                def weigh(src, dst, total_ref):
                    diag = jnp.where(causal, src[:, prev:length], -jnp.inf)
                    peak = jnp.max(diag, axis=-1, keepdims=True)
                    if prev:
                        peak = jnp.maximum(peak, jnp.max(src[:, :prev], axis=-1, keepdims=True))
                    e_diag = jnp.exp2((diag - peak) * scale)
                    total = jnp.sum(e_diag, axis=-1, keepdims=True)
                    dst[:, prev:length] = e_diag.astype(jnp.bfloat16)
                    if prev:
                        e_past = jnp.exp2((src[:, :prev] - peak) * scale)
                        total = total + jnp.sum(e_past, axis=-1, keepdims=True)
                        dst[:, :prev] = e_past.astype(jnp.bfloat16)
                    total_ref[...] = jnp.broadcast_to(total, total_ref.shape)

                def mix(head, src, total_ref):
                    cols = pl.ds(pl.multiple_of(head * NOPE_DIM, NOPE_DIM), NOPE_DIM)
                    mixed = jnp.dot(src[:, :length], v_s[:length, cols], preferred_element_type=jnp.float32)
                    o_s[:, cols] = (mixed / total_ref[...]).astype(jnp.bfloat16)

                def quad(idx, carry):
                    for head in (idx * 4, idx * 4 + 2):
                        score(head + 1, 1, s1_s)
                        weigh(s0_s, p0_s, t0_s)
                        mix(jnp.maximum(head - 1, 0), p1_s, t1_s)
                        score(jnp.minimum(head + 2, n_heads - 2), 0, s0_s)
                        weigh(s1_s, p1_s, t1_s)
                        mix(head, p0_s, t0_s)
                    return carry

                score(0, 0, s0_s)
                lax.fori_loop(0, n_heads // 4, quad, 0)
                mix(n_heads - 1, p1_s, t1_s)

        y = jnp.dot(o_s[:, :half], wo_own[...], preferred_element_type=jnp.float32)
        y = y + jnp.dot(o_s[:, half:], wo_oth[...], preferred_element_type=jnp.float32)
        y = y.astype(jnp.bfloat16)
        if ret_ref is not None:
            @pl.when(req < n_ret)
            def _():
                ret_ref[0] = y

        @pl.when(jnp.logical_not(is_far))
        def _():
            out_ref[0] = y

    @pl.when(jnp.logical_not(jnp.logical_and(active, jnp.logical_not(is_far))))
    def _():
        out_ref[0] = jnp.zeros(out_ref.shape[1:], out_ref.dtype)


def attend(ids, flags, hidden, recv, weights, out_prev, n_ret):
    n_req = ids.shape[0]
    _, seq_len, width = hidden.shape
    w_dkv, gain, wq_own, wq_oth, kv_own, kv_oth, wo_own, wo_oth, _, _ = weights
    n_blocks = seq_len // BLOCK
    kv_rank = gain.shape[1]
    half = wo_own.shape[0]
    lat_width = kv_rank + ROPE_DIM
    whole = lambda arr: pl.BlockSpec(arr.shape, lambda r, i, ids, flags: (0, 0), pipeline_mode=pl.Buffered(1))
    in_specs = [
        pl.BlockSpec((1, BLOCK, width), lambda r, i, ids, flags: (jnp.where(flags[0] == 1, 0, ids[r]), jnp.where(flags[0] == 1, 0, i), 0)),
        pl.BlockSpec((1, BLOCK, width), lambda r, i, ids, flags: (0, jnp.where((flags[0] == 1) & (r == 0), i, 0), 0)),
        *[whole(arr) for arr in (w_dkv, gain, wq_own, wq_oth, kv_own, kv_oth, wo_own, wo_oth)],
        pl.BlockSpec((BLOCK, LANES), lambda r, i, ids, flags: (i, 0)),
        pl.BlockSpec((BLOCK, LANES), lambda r, i, ids, flags: (i, 0)),
    ]
    args = [hidden, recv, *weights]
    out_shape = [jax.ShapeDtypeStruct(hidden.shape, jnp.bfloat16), jax.ShapeDtypeStruct((n_req, seq_len, lat_width), jnp.bfloat16)]
    out_specs = [
        pl.BlockSpec((1, BLOCK, width), lambda r, i, ids, flags: (ids[r], i, 0)),
        pl.BlockSpec((1, BLOCK, lat_width), lambda r, i, ids, flags: (r, i, 0)),
    ]
    if n_ret:
        out_shape.append(jax.ShapeDtypeStruct((n_ret, seq_len, width), jnp.bfloat16))
        out_specs.append(pl.BlockSpec((1, BLOCK, width), lambda r, i, ids, flags: (jnp.minimum(r, n_ret - 1), jnp.where(r < n_ret, i, n_blocks - 1), 0)))
    aliases = {}
    if out_prev is not None:
        in_specs.append(pl.BlockSpec(memory_space=pl.ANY))
        args.append(out_prev)
        aliases = {2 + len(args) - 1: 0}
    flops = n_req * seq_len * (2 * width * (768 + 3 * half * 2 // 2 * 1 + 2 * half) + 8 * kv_rank * half + 2 * half * seq_len * 3)
    outs = pl.pallas_call(
        functools.partial(attend_kernel, n_ret, out_prev is not None),
        out_shape=out_shape,
        grid_spec=pltpu.PrefetchScalarGridSpec(
            num_scalar_prefetch=2,
            grid=(n_req, n_blocks),
            in_specs=in_specs,
            out_specs=out_specs,
            scratch_shapes=[
                pltpu.VMEM((BLOCK, width), jnp.bfloat16),
                pltpu.VMEM((seq_len, 2 * half), jnp.bfloat16),
                pltpu.VMEM((seq_len, 2 * half), jnp.bfloat16),
                pltpu.VMEM((seq_len, 2 * LANES), jnp.bfloat16),
                pltpu.VMEM((BLOCK, 2 * half), jnp.bfloat16),
                pltpu.VMEM((BLOCK, half), jnp.bfloat16),
                pltpu.VMEM((BLOCK, 2 * half), jnp.bfloat16),
                *[pltpu.VMEM((BLOCK, seq_len), jnp.float32)] * 2,
                *[pltpu.VMEM((BLOCK, seq_len), jnp.bfloat16)] * 2,
                *[pltpu.VMEM((BLOCK, NOPE_DIM), jnp.float32)] * 2,
            ],
        ),
        input_output_aliases=aliases,
        compiler_params=pltpu.CompilerParams(dimension_semantics=("arbitrary", "arbitrary"), vmem_limit_bytes=66_000_000),
        cost_estimate=pl.CostEstimate(flops=flops, bytes_accessed=n_req * seq_len * width * 6, transcendentals=n_req * seq_len * seq_len * 8),
        name="attend",
    )(ids, flags, *args)
    return outs if n_ret else (*outs, None)


def solution(mesh):
    n_stage = mesh.shape["stage"]
    half_stage = n_stage // 2
    down = [(idx, idx + half_stage) for idx in range(half_stage)]
    up = [(idx + half_stage, idx) for idx in range(half_stage)]
    cores = [(idx, idx ^ 1) for idx in range(n_stage)]
    swap = [(0, 1), (1, 0)]
    slot_spec = P(("dp", "stage"), None, None, None)
    cache_spec = P(("dp", "stage"), "t", None, None)

    def other_half(arr, core):
        rows = arr.shape[0] // 2
        mine = lax.ppermute(lax.dynamic_slice_in_dim(arr, core * rows, rows, axis=0), "t", swap)
        theirs = lax.ppermute(mine, "stage", cores)
        first = jnp.where(core == 0, mine, theirs)
        second = jnp.where(core == 0, theirs, mine)
        return jnp.concatenate([first, second], axis=0)

    def device_step(hidden, w_query, w_dkv, latent_gain, w_uk, w_uv, w_out):
        tokens = hidden[0]
        n_all, seq_len, width = tokens.shape
        kv_rank = latent_gain.shape[0]
        n_half = n_all // 2
        t_index = lax.axis_index("t")
        stage = lax.axis_index("stage")
        is_prompt = stage < half_stage
        core = stage % 2
        own, oth = t_index * n_half, (1 - t_index) * n_half

        arrivals = []
        for idx in range(N_FAR):
            index = own + idx
            if idx > 1:
                index, _ = lax.optimization_barrier((index, arrivals[-2]))
            piece = lax.dynamic_slice_in_dim(tokens, index, 1, axis=0)
            if arrivals:
                piece, _ = lax.optimization_barrier((piece, arrivals[-1]))
            arrivals.append(lax.ppermute(piece, "stage", down))

        heads_here = w_uk.shape[1] // NOPE_DIM
        wq = w_query.reshape(width, heads_here, NOPE_DIM + ROPE_DIM)
        wq_own = jnp.concatenate([wq[:, :, :NOPE_DIM].reshape(width, -1), wq[:, :, NOPE_DIM:].reshape(width, -1)], axis=1)
        kv_own = jnp.concatenate([w_uk, w_uv], axis=1)
        wo_oth, kv_oth, wq_oth = other_half(w_out, core), other_half(kv_own, core), other_half(wq_own, core)
        blank = jnp.zeros((width, ROPE_DIM), w_dkv.dtype)
        w_dkv_wide = jnp.concatenate([w_dkv, blank, blank, w_dkv[:, kv_rank:]], axis=1)
        gain = latent_gain.astype(jnp.float32)[None, :]
        weights = (w_dkv_wide, gain, wq_own, wq_oth, kv_own, kv_oth, w_out, wo_oth, *rope_tables(seq_len))

        ids = jnp.concatenate([own + jnp.arange(N_FAR, n_half), oth + jnp.arange(N_FAR + N_SWAP, n_half)]).astype(jnp.int32)
        far = jnp.where(is_prompt, 0, 1).astype(jnp.int32)
        place = lambda out, block, index: lax.dynamic_update_slice(out, jnp.where(is_prompt, block, jnp.zeros_like(block)), (index, 0, 0))

        out, done = None, 0
        latents, far_latents = [], []
        backs, movements = {}, {}

        def put(idx, source):
            nonlocal out
            for block, index in source.pop(idx, ()):
                out = place(out, block, index)

        def run(count, recv, n_ret, far_active):
            nonlocal out, done
            flags = jnp.stack([far, *[jnp.where(is_prompt, 1, 1 if far_active and idx == 0 else 0).astype(jnp.int32) for idx in range(count)]])
            out, lat, ret = attend(ids[done:done + count], flags, tokens, recv, weights, out, n_ret)
            n_send = max(0, min(count, n_half - N_FAR - done))
            if n_send:
                sent, _ = lax.optimization_barrier((lat[:n_send], arrivals[-1]))
                latents.append(lax.ppermute(sent, "stage", down))
            if far_active:
                far_latents.append(lat[:1])
            done += count
            return ret

        n_steps = len(STEP_CALLS)
        for idx, count in enumerate(STEP_CALLS):
            put(idx - 2, backs)
            put(idx - 4, movements)
            ret = run(count, arrivals[idx], 1, True)
            if idx < N_SWAP:
                swapped = lax.ppermute(ret, "t", swap)
            back = lax.ppermute(ret, "stage", up)
            moved = lax.ppermute(back, "t", swap)
            backs[idx] = [(back, own + idx)]
            movements[idx] = [(moved, oth + idx)]
            if idx < N_SWAP:
                movements[idx].append((swapped, oth + N_FAR + idx))
        for idx, count in enumerate(TAIL_CALLS):
            put(n_steps + idx - 2, backs)
            put(n_steps + idx - 4, movements)
            run(count, tokens, 0, False)
        for idx in range(n_steps):
            put(idx, backs)
            put(idx, movements)
        pieces = [*far_latents, *latents]

        def empty(parts):
            return with_layout_constraint(jnp.zeros((n_half, kv_rank + ROPE_DIM, seq_len), jnp.bfloat16), Layout((0, 1, 2)))

        def gathered(parts):
            return with_layout_constraint(jnp.swapaxes(jnp.concatenate(parts, axis=0), 1, 2), Layout((0, 1, 2)))

        latent = jnp.swapaxes(lax.cond(is_prompt, empty, gathered, pieces), 1, 2)
        return out[None], latent[None]

    in_specs = (slot_spec, P(None, "t"), P(None, None), P(None), P(None, "t"), P(None, "t"), P("t", None))
    return jax.shard_map(device_step, mesh=mesh, in_specs=in_specs, out_specs=(slot_spec, cache_spec), check_vma=False)
```
